32 devices in a mesh: gz: 4 (over z), gy: 4 (over y, x), gx: 2 (over core).
Axes of the slice: x: 2, y: 2, z: 4, core: 2. Of those that a mesh axis runs over, the one named last changes fastest.
Arguments:
- right_side: float32 [32, 64, 256], P('gz', 'gy', 'gx'), may hold values from -128 to 128
- diagonal: float32 [32, 64, 256], P('gz', 'gy', 'gx'), may hold values from 0.05 to 1
Outputs:
- solution_field: float32 [32, 64, 256], P('gz', 'gy', 'gx')
- residual: float32 [32, 64, 256], P('gz', 'gy', 'gx')
The draws below stay inside these ranges and needn't reach their ends.
All inputs are finite; a program needn't handle non-finite values.
Results may differ from the reference program's by a relative error of at most 0.03.
Values sent between devices are 32-bit elements.
A program may use at most 64 MiB of HBM per device.

```python
import jax
import jax.numpy as jnp
import numpy as np
from jax import lax

S = 6
OUTER = 5
NZ = 32
NY = 64
NX = 256


def shard_levels(own_key, dims, pieces, low, largest):
    factor_of = 1.0
    for position, blocks in pieces:
        steps = jax.random.uniform(jax.random.fold_in(jax.random.fold_in(own_key, 6), position), (blocks,), jnp.float32, low / len(pieces), largest / len(pieces))
        factor_of = factor_of * jnp.repeat(jnp.exp(steps), dims[position] // blocks).reshape((-1,) + (1,) * (len(dims) - 1 - position))
    return factor_of


def gaussian(own_key, extent, spread, most, split=(), kind=jnp.bfloat16):
    result = spread * jax.random.normal(own_key, extent, jnp.float32)
    if split:
        result = result * shard_levels(own_key, extent, split, -0.22, 0.18)
    return jnp.clip(result, -most, most).astype(kind)


def setup_inputs(seed: int = 0) -> dict:
    key_list = jax.random.split(jax.random.key(seed), 3)
    return {
        "right_side": gaussian(key_list[0], (NZ, NY, NX), 24.0, 128.0, ((0, 4), (1, 4), (2, 2)), jnp.float32),
        "diagonal": jnp.clip(0.05 + 0.95 * jax.random.uniform(key_list[1], (NZ, NY, NX), jnp.float32) ** shard_levels(key_list[1], (NZ, NY, NX), ((0, 4), (1, 4), (2, 2)), -0.2, 0.2), 0.05, 1.0),
    }


center_shift = 19.0
half_width = 19.0


def apply_operator(padded, diagonal):
    extent_z = padded.shape[-3] - 2
    extent_y = padded.shape[-2] - 2
    extent_x = padded.shape[-1] - 2
    running = jnp.zeros(padded[..., 1:-1, 1:-1, 1:-1].shape, jnp.float32)
    for along_z in range(3):
        for along_y in range(3):
            for along_x in range(3):
                if along_z == 1 and along_y == 1 and along_x == 1:
                    continue
                running = running + padded[..., along_z:along_z + extent_z, along_y:along_y + extent_y, along_x:along_x + extent_x]
    return (26.0 + diagonal) * padded[..., 1:-1, 1:-1, 1:-1] - running


def chebyshev_next(images, current, previous):
    scaled = (images - center_shift * current) / half_width
    if previous is None:
        return scaled
    return 2.0 * scaled - previous


def basis_change():
    columns = 2 * S + 1
    matrix = np.zeros((columns, columns), np.float32)
    for offset, length in ((0, S), (S + 1, S - 1)):
        for degree in range(length):
            matrix[offset + degree, offset + degree] = center_shift
            if degree == 0:
                matrix[offset + 1, offset] = half_width
            else:
                matrix[offset + degree + 1, offset + degree] = 0.5 * half_width
                matrix[offset + degree - 1, offset + degree] = 0.5 * half_width
    return matrix


def coefficients(gram_matrix):
    columns = 2 * S + 1
    change = jnp.asarray(basis_change(), dtype=jnp.float32)
    identity = jnp.eye(columns, dtype=jnp.float32)
    dir_coeff = identity[0]
    res_coeff = identity[S + 1]
    sol_coeff = jnp.zeros((columns,), jnp.float32)
    for degree in range(S):
        moved = jnp.dot(change, dir_coeff, precision=lax.Precision.HIGHEST)
        norm_now = jnp.dot(res_coeff, jnp.dot(gram_matrix, res_coeff, precision=lax.Precision.HIGHEST), precision=lax.Precision.HIGHEST)
        curvature = jnp.dot(dir_coeff, jnp.dot(gram_matrix, moved, precision=lax.Precision.HIGHEST), precision=lax.Precision.HIGHEST)
        step_len = norm_now / curvature
        sol_coeff = sol_coeff + step_len * dir_coeff
        res_next = res_coeff - step_len * moved
        norm_next = jnp.dot(res_next, jnp.dot(gram_matrix, res_next, precision=lax.Precision.HIGHEST), precision=lax.Precision.HIGHEST)
        dir_coeff = res_next + (norm_next / norm_now) * dir_coeff
        res_coeff = res_next
    return sol_coeff, res_coeff, dir_coeff


def combine(coeff, basis_set):
    return jnp.tensordot(coeff, basis_set, axes=1, precision=lax.Precision.HIGHEST)


def reference(right_side, diagonal):
    solution = jnp.zeros(right_side.shape, jnp.float32)
    residual = right_side
    direction = right_side
    for outer_step in range(OUTER):
        p_fields = [direction]
        for degree in range(S):
            images = apply_operator(jnp.pad(p_fields[-1], 1), diagonal)
            p_fields.append(chebyshev_next(images, p_fields[-1], p_fields[-2] if degree else None))
        r_fields = [residual]
        for degree in range(S - 1):
            images = apply_operator(jnp.pad(r_fields[-1], 1), diagonal)
            r_fields.append(chebyshev_next(images, r_fields[-1], r_fields[-2] if degree else None))
        basis_set = jnp.stack(p_fields + r_fields)
        flattened = basis_set.reshape(basis_set.shape[0], -1)
        gram_matrix = jnp.dot(flattened, flattened.T, precision=lax.Precision.HIGHEST)
        sol_coeff, res_coeff, dir_coeff = coefficients(gram_matrix)
        solution = solution + combine(sol_coeff, basis_set)
        residual = combine(res_coeff, basis_set)
        direction = combine(dir_coeff, basis_set)
    return solution, residual
```

```python
import jax
import jax.numpy as jnp
import numpy as np
from jax import lax
from jax.experimental import pallas as pl
from jax.experimental.pallas import tpu as pltpu
from jax.sharding import PartitionSpec as P

S = 6
OUTER = 5
COLS = 2 * S + 1
SHIFT = 19.0
HALF = 19.0
LANES = 128
ROWS = 8
MESH = pl.DeviceIdType.MESH


def basis_change():
    matrix = np.zeros((COLS, COLS), np.float32)
    for offset, length in ((0, S), (S + 1, S - 1)):
        for degree in range(length):
            matrix[offset + degree, offset + degree] = SHIFT
            if degree == 0:
                matrix[offset + 1, offset] = HALF
            else:
                matrix[offset + degree + 1, offset + degree] = 0.5 * HALF
                matrix[offset + degree - 1, offset + degree] = 0.5 * HALF
    return matrix


def table(index, values):
    out = jnp.zeros(index.shape, jnp.float32)
    for position, value in enumerate(values):
        if value:
            out = jnp.where(index == position, jnp.float32(value), out)
    return out


def kernel(nz, ny, nx, rhs_ref, diag_ref, sol_out, res_out,
           fields, p_chain, r_chain, scale2, weight, total, pairs, g_send, g_recv, final,
           z_send, z_recv, y_send, y_recv, g_ssem, g_rsem, swap_send, swap_recv, own_sem):
    bz, by, bx = rhs_ref.shape
    hy = by // 2
    ze, halves, ya = fields.shape[1:4]
    first = (ya - hy) // 2
    low_rows, high_rows = slice(first - ROWS, first), slice(first + hy, first + hy + ROWS)
    iz, iy, ix = lax.axis_index("gz"), lax.axis_index("gy"), lax.axis_index("gx")
    other = 1 - ix
    yy = iy * 2 + ix
    count = nz * ny * nx
    me = (iz * ny + iy) * nx + ix
    has_z = (iz > 0, iz < nz - 1)
    has_y = (yy > 0, yy < 2 * ny - 1)
    z_dev = tuple((iz + s, iy, ix) for s in (-1, 1))
    y_dev = tuple((iz, (yy + s) // 2, other) for s in (-1, 1))
    mid_z, mid_y = slice(S, S + bz), slice(first, first + hy)

    def row_tile(index):
        return pl.ds(pl.multiple_of(index * hy, hy), hy)

    swaps, owns = [], []
    for k, ref in enumerate((rhs_ref, diag_ref)):
        spot = fields.at[1 + k, mid_z, ix, mid_y, :]
        swap = pltpu.make_async_remote_copy(
            src_ref=ref.at[:, row_tile(other), :], dst_ref=spot,
            send_sem=swap_send.at[k], recv_sem=swap_recv.at[k],
            device_id=(iz, iy, other), device_id_type=MESH)
        swap.start()
        own = pltpu.make_async_copy(ref.at[:, row_tile(ix), :], spot, own_sem.at[k])
        own.start()
        swaps.append(swap)
        owns.append(own)

    for side in range(2):
        planes = slice(0, S) if side == 0 else slice(S + bz, ze)
        rows = (low_rows, high_rows)[side]

        @pl.when(jnp.logical_not(has_z[side]))
        def _():
            for k in (0, 1, 2):
                fields[k, planes] = jnp.zeros((S, halves, ya, bx), jnp.float32)

        @pl.when(jnp.logical_not(has_y[side]))
        def _():
            for k in (0, 1, 2):
                fields[k, :, :, rows, :] = jnp.zeros((ze, halves, ROWS, bx), jnp.float32)

    w_unit = 2.0 / HALF
    w_low = jnp.where(has_y[0], jnp.float32(w_unit), 0.0)
    w_high = jnp.where(has_y[1], jnp.float32(w_unit), 0.0)
    z_low = jnp.where(has_z[0], jnp.float32(1.0), 0.0)
    z_high = jnp.where(has_z[1], jnp.float32(1.0), 0.0)
    for plane in range(ze):
        factor = z_low if plane < S else (z_high if plane >= S + bz else jnp.float32(1.0))
        for tile, w in enumerate((w_low, jnp.float32(w_unit), w_high)):
            weight[plane, tile] = jnp.broadcast_to(w * factor, (ROWS, bx))
    total[...] = jnp.zeros(total.shape, jnp.float32)
    pairs[...] = jnp.zeros(pairs.shape, jnp.float32)

    for copy in owns + swaps:
        copy.wait()

    def z_copy(lo, side):
        src = slice(S, 2 * S) if side == 0 else slice(bz, bz + S)
        dst = slice(S + bz, ze) if side == 0 else slice(0, S)
        return pltpu.make_async_remote_copy(
            src_ref=fields.at[lo:lo + 2, src, :, mid_y, :], dst_ref=fields.at[lo:lo + 2, dst, :, mid_y, :],
            send_sem=z_send.at[side], recv_sem=z_recv.at[1 - side],
            device_id=z_dev[side], device_id_type=MESH)

    def y_copy(lo, side, part):
        planes = (mid_z, slice(0, S), slice(S + bz, ze))[part]
        dst = (high_rows, low_rows)[side]
        return pltpu.make_async_remote_copy(
            src_ref=fields.at[lo:lo + 2, planes, :, mid_y, :], dst_ref=fields.at[lo:lo + 2, planes, :, dst, :],
            send_sem=y_send.at[side, part], recv_sem=y_recv.at[1 - side, part],
            device_id=y_dev[side], device_id_type=MESH)

    def exchange(lo):
        for side in range(2):
            @pl.when(has_z[side])
            def _():
                z_copy(lo, side).start()
        for side in range(2):
            @pl.when(has_y[side])
            def _():
                y_copy(lo, side, 0).start()
        for z_side in range(2):
            @pl.when(has_z[z_side])
            def _():
                z_copy(lo, 1 - z_side).wait_recv()
                for side in range(2):
                    @pl.when(has_y[side])
                    def _():
                        y_copy(lo, side, 1 + z_side).start()
        for side in range(2):
            @pl.when(has_z[side])
            def _():
                z_copy(lo, side).wait_send()

            @pl.when(has_y[side])
            def _():
                y_copy(lo, side, 0).wait_send()
                y_copy(lo, 1 - side, 0).wait_recv()
                for z_side in range(2):
                    @pl.when(has_z[z_side])
                    def _():
                        y_copy(lo, side, 1 + z_side).wait_send()
                        y_copy(lo, 1 - side, 1 + z_side).wait_recv()

    exchange(1)
    all_rows = slice(first - ROWS, first + hy + ROWS)

    def prepare(plane, c):
        fields[0, plane] = fields[1, plane]
        scale2[plane] = (fields[2, plane, :, all_rows, :] + (27.0 - SHIFT)) * (2.0 / HALF)
        return c
    lax.fori_loop(0, ze, prepare, 0)

    tiles = (hy + 2 * ROWS) // ROWS
    lane_id = lax.broadcasted_iota(jnp.int32, (ROWS, bx), 1)
    first_lane, last_lane = lane_id == 0, lane_id == bx - 1

    def row_sums(ref, z, tile):
        at = first - ROWS + tile * ROWS
        return [ref[z, h, at - 1:at - 1 + ROWS, :] + ref[z, h, at:at + ROWS, :] + ref[z, h, at + 1:at + 1 + ROWS, :]
                for h in range(halves)]

    def lane_sums(parts):
        left = [pltpu.roll(v, 1, 1) for v in parts]
        right = [pltpu.roll(v, bx - 1, 1) for v in parts]
        out = []
        for h in range(halves):
            before = left[h - 1] if h else 0.0
            after = right[h + 1] if h < halves - 1 else 0.0
            out.append(parts[h] + jnp.where(first_lane, before, left[h]) + jnp.where(last_lane, after, right[h]))
        return out

    p_at = [fields.at[1]] + [p_chain.at[k] for k in range(S)]
    r_at = [fields.at[0]] + [r_chain.at[k] for k in range(S - 1)]

    def degree_sweep(chains, degree, start, stop, chosen):
        jobs = [(chain, tile) for chain in chains for tile in chosen]

        def step(z, carry):
            out = []
            for (chain, tile), (before, here) in zip(jobs, carry):
                after = row_sums(chain[degree], z + 1, tile)
                box = lane_sums([a + b + c for a, b, c in zip(before, here, after)])
                at = first - ROWS + tile * ROWS
                for h in range(halves):
                    value = (scale2[z, h, tile * ROWS:(tile + 1) * ROWS, :] * chain[degree][z, h, at:at + ROWS, :]
                             - weight[z, tile] * box[h])
                    if degree == 0:
                        value = 0.5 * value
                    else:
                        value = value - chain[degree - 1][z, h, at:at + ROWS, :]
                    chain[degree + 1][z, h, at:at + ROWS, :] = value
                out.append((here, after))
            return tuple(out)
        init = tuple((row_sums(c[degree], start - 1, k), row_sums(c[degree], start, k)) for c, k in jobs)
        for z in range(start, stop):
            init = step(z, init)

    gl = lax.broadcasted_iota(jnp.int32, (2 * ROWS, LANES), 1)
    gr = lax.broadcasted_iota(jnp.int32, (2 * ROWS, LANES), 0)
    change = basis_change()
    diag_b = [change[i, i] for i in range(COLS)]
    low_b = [change[i, i - 1] if i else 0.0 for i in range(COLS)]
    up_b = [change[i, i + 1] if i < COLS - 1 else 0.0 for i in range(COLS)]
    b_row = [table(gl, v) for v in (diag_b, low_b, up_b)]
    b_col = [table(gr, v) for v in (diag_b, low_b, up_b)]

    def apply_b(col, row):
        q_row = b_row[0] * row + b_row[1] * pltpu.roll(row, 1, 1) + b_row[2] * pltpu.roll(row, LANES - 1, 1)
        q_col = b_col[0] * col + b_col[1] * pltpu.roll(col, 1, 0) + b_col[2] * pltpu.roll(col, 2 * ROWS - 1, 0)
        return q_col, q_row

    def outer(t, carry):
        for degree in range(S):
            if degree < S - 1:
                degree_sweep((p_at,), degree, degree + 1, ze - degree - 1, range(tiles))
                r_tiles = range(tiles) if degree < S - 2 else (1,)
                degree_sweep((r_at,), degree, degree + 2, ze - degree - 2, r_tiles)
            else:
                degree_sweep((p_at,), degree, degree + 1, ze - degree - 1, (1,))
        basis = p_at + r_at

        for lo_i, hi_i, lo_j in ((0, S + 1, 0), (0, S + 1, S + 1), (S + 1, COLS, S + 1)):
            hi_j = S + 1 if lo_j == 0 else COLS
            sums = {}
            for z in range(S, S + bz):
                for h in range(halves):
                    va = [basis[i][z, h, mid_y, :] for i in range(lo_i, hi_i)]
                    vb = va if lo_i == lo_j else [basis[j][z, h, mid_y, :] for j in range(lo_j, hi_j)]
                    for i in range(lo_i, hi_i):
                        for j in range(max(i, lo_j), hi_j):
                            term = va[i - lo_i] * vb[j - lo_j]
                            sums[i, j] = sums[i, j] + term if (i, j) in sums else term
            for (i, j), value in sums.items():
                line = jnp.sum(value, axis=0, keepdims=True)
                pairs[i * 16 + j:i * 16 + j + 1, :] = line
                if i != j:
                    pairs[j * 16 + i:j * 16 + i + 1, :] = line
        for half in range(2):
            turned = pairs[half * LANES:(half + 1) * LANES, :].T
            g_send[half:half + 1, :] = jnp.sum(turned, axis=0, keepdims=True)

        slot = t % 2
        own = pltpu.make_async_copy(g_send, g_recv.at[slot, me], g_rsem.at[slot])
        own.start()

        def send(d, c):
            peer = (me + d) % count
            pltpu.make_async_remote_copy(
                src_ref=g_send, dst_ref=g_recv.at[slot, me],
                send_sem=g_ssem, recv_sem=g_rsem.at[slot],
                device_id=(peer // (ny * nx), (peer // nx) % ny, peer % nx), device_id_type=MESH).start()
            return c
        lax.fori_loop(1, count, send, 0)
        everything = g_recv.at[slot]
        pltpu.make_async_copy(everything, everything, g_rsem.at[slot]).wait()
        most = g_recv.at[slot, 0:count - 1]
        pltpu.make_async_copy(most, most, g_ssem).wait()
        rows2 = jnp.sum(g_recv[slot], axis=0)
        gram = jnp.zeros((2 * ROWS, LANES), jnp.float32)
        for half in range(2):
            line = jnp.broadcast_to(rows2[half:half + 1, :], (2 * ROWS, LANES))
            for k in range(8):
                i = half * 8 + k
                if i < COLS:
                    moved = line if k == 0 else pltpu.roll(line, LANES - 16 * k, 1)
                    gram = jnp.where(gr == i, moved, gram)
        gram = jnp.where(gl < COLS, gram, 0.0)

        def quad(col, row):
            return jnp.sum(jnp.sum(gram * col * row, axis=0, keepdims=True), axis=1, keepdims=True)

        p_row, p_col = (gl == 0).astype(jnp.float32), (gr == 0).astype(jnp.float32)
        r_row, r_col = (gl == S + 1).astype(jnp.float32), (gr == S + 1).astype(jnp.float32)
        x_col = jnp.zeros((2 * ROWS, LANES), jnp.float32)
        norm = quad(r_col, r_row)
        for _ in range(S):
            q_col, q_row = apply_b(p_col, p_row)
            length = norm / quad(p_col, q_row)
            x_col = x_col + length * p_col
            r_col = r_col - length * q_col
            r_row = r_row - length * q_row
            fresh = quad(r_col, r_row)
            ratio = fresh / norm
            p_col = r_col + ratio * p_col
            p_row = r_row + ratio * p_row
            norm = fresh

        def weights(col):
            return [jnp.broadcast_to(col[i:i + 1, :], (hy, LANES)) for i in range(COLS)]

        xw, rw, pw = weights(x_col), weights(r_col), weights(p_col)
        for z in range(bz):
            for h in range(halves):
                vs = [b[S + z, h, mid_y, :] for b in basis]

                def mix(w):
                    out = w[0] * vs[0]
                    for a, b in zip(w[1:], vs[1:]):
                        out = out + a * b
                    return out
                total[0, z, h] = total[0, z, h] + mix(xw)
                fields[0, S + z, h, mid_y, :] = mix(rw)
                fields[1, S + z, h, mid_y, :] = mix(pw)

        @pl.when(t < OUTER - 1)
        def _():
            exchange(0)
        return carry

    lax.fori_loop(0, OUTER, outer, 0)

    total[1] = fields[0, mid_z, :, mid_y, :]
    back = pltpu.make_async_remote_copy(
        src_ref=total.at[:, :, other], dst_ref=final,
        send_sem=swap_send.at[0], recv_sem=swap_recv.at[0],
        device_id=(iz, iy, other), device_id_type=MESH)
    back.start()
    for k, out in enumerate((sol_out, res_out)):
        out[:, row_tile(ix), :] = total[k, :, ix]
    back.wait()
    for k, out in enumerate((sol_out, res_out)):
        out[:, row_tile(other), :] = final[k]


def solution(mesh):
    nz, ny, nx = mesh.shape["gz"], mesh.shape["gy"], mesh.shape["gx"]
    count = nz * ny * nx

    def body(right_side, diagonal):
        bz, by, bx = right_side.shape
        hy = by // 2
        assert nx == 2 and bz >= S and hy == ROWS and bx == LANES
        ze, ye = bz + 2 * S, hy + 4 * ROWS
        f32, dma = jnp.float32, pltpu.SemaphoreType.DMA
        return pl.pallas_call(
            lambda *refs: kernel(nz, ny, nx, *refs),
            out_shape=(jax.ShapeDtypeStruct(right_side.shape, f32),) * 2,
            in_specs=[pl.BlockSpec(memory_space=pltpu.VMEM)] * 2,
            out_specs=(pl.BlockSpec(memory_space=pltpu.VMEM),) * 2,
            scratch_shapes=[
                pltpu.VMEM((3, ze, nx, ye, bx), f32),
                pltpu.VMEM((S, ze, nx, ye, bx), f32),
                pltpu.VMEM((S - 1, ze, nx, ye, bx), f32),
                pltpu.VMEM((ze, nx, hy + 2 * ROWS, bx), f32),
                pltpu.VMEM((ze, 3, ROWS, bx), f32),
                pltpu.VMEM((2, bz, nx, hy, bx), f32),
                pltpu.VMEM((2 * LANES, LANES), f32),
                pltpu.VMEM((2, LANES), f32),
                pltpu.VMEM((2, count, 2, LANES), f32),
                pltpu.VMEM((2, bz, hy, bx), f32),
                dma((2,)), dma((2,)), dma((2, 3)), dma((2, 3)),
                dma, dma((2,)), dma((2,)), dma((2,)), dma((2,)),
            ],
            compiler_params=pltpu.CompilerParams(has_side_effects=True),
        )(right_side, diagonal)

    spec = P("gz", "gy", "gx")
    return jax.shard_map(body, mesh=mesh, in_specs=(spec, spec), out_specs=(spec, spec), check_vma=False)
```

```python
import jax
import jax.numpy as jnp
import numpy as np
from jax import lax
from jax.experimental import pallas as pl
from jax.experimental.pallas import tpu as pltpu
from jax.sharding import PartitionSpec as P

S = 6
OUTER = 5
COLS = 2 * S + 1
SHIFT = 19.0
HALF = 19.0
LANES = 128
ROWS = 8
MESH = pl.DeviceIdType.MESH


def basis_change():
    matrix = np.zeros((COLS, COLS), np.float32)
    for offset, length in ((0, S), (S + 1, S - 1)):
        for degree in range(length):
            matrix[offset + degree, offset + degree] = SHIFT
            if degree == 0:
                matrix[offset + 1, offset] = HALF
            else:
                matrix[offset + degree + 1, offset + degree] = 0.5 * HALF
                matrix[offset + degree - 1, offset + degree] = 0.5 * HALF
    return matrix


def table(index, values):
    out = jnp.zeros(index.shape, jnp.float32)
    for position, value in enumerate(values):
        if value:
            out = jnp.where(index == position, jnp.float32(value), out)
    return out


def kernel(nz, ny, nx, rhs_ref, diag_ref, sol_out, res_out,
           fields, p_chain, r_chain, scale2, weight, total, pairs, g_send, g_recv, final,
           z_send, z_recv, y_send, y_recv, g_ssem, g_rsem, swap_send, swap_recv, own_sem):
    bz, by, bx = rhs_ref.shape
    hy = by // 2
    ze, halves, ya = fields.shape[1:4]
    first = (ya - hy) // 2
    low_rows, high_rows = slice(first - ROWS, first), slice(first + hy, first + hy + ROWS)
    iz, iy, ix = lax.axis_index("gz"), lax.axis_index("gy"), lax.axis_index("gx")
    other = 1 - ix
    yy = iy * 2 + ix
    count = nz * ny * nx
    me = (iz * ny + iy) * nx + ix
    has_z = (iz > 0, iz < nz - 1)
    has_y = (yy > 0, yy < 2 * ny - 1)
    z_dev = tuple((iz + s, iy, ix) for s in (-1, 1))
    y_dev = tuple((iz, (yy + s) // 2, other) for s in (-1, 1))
    mid_z, mid_y = slice(S, S + bz), slice(first, first + hy)

    def row_tile(index):
        return pl.ds(pl.multiple_of(index * hy, hy), hy)

    swaps, owns = [], []
    for k, ref in enumerate((rhs_ref, diag_ref)):
        spot = fields.at[1 + k, mid_z, ix, mid_y, :]
        swap = pltpu.make_async_remote_copy(
            src_ref=ref.at[:, row_tile(other), :], dst_ref=spot,
            send_sem=swap_send.at[k], recv_sem=swap_recv.at[k],
            device_id=(iz, iy, other), device_id_type=MESH)
        swap.start()
        own = pltpu.make_async_copy(ref.at[:, row_tile(ix), :], spot, own_sem.at[k])
        own.start()
        swaps.append(swap)
        owns.append(own)

    for side in range(2):
        planes = slice(0, S) if side == 0 else slice(S + bz, ze)
        rows = (low_rows, high_rows)[side]

        @pl.when(jnp.logical_not(has_z[side]))
        def _():
            for k in (0, 1, 2):
                fields[k, planes] = jnp.zeros((S, halves, ya, bx), jnp.float32)

        @pl.when(jnp.logical_not(has_y[side]))
        def _():
            for k in (0, 1, 2):
                fields[k, :, :, rows, :] = jnp.zeros((ze, halves, ROWS, bx), jnp.float32)

    w_unit = 2.0 / HALF
    w_low = jnp.where(has_y[0], jnp.float32(w_unit), 0.0)
    w_high = jnp.where(has_y[1], jnp.float32(w_unit), 0.0)
    z_low = jnp.where(has_z[0], jnp.float32(1.0), 0.0)
    z_high = jnp.where(has_z[1], jnp.float32(1.0), 0.0)
    for plane in range(ze):
        factor = z_low if plane < S else (z_high if plane >= S + bz else jnp.float32(1.0))
        for tile, w in enumerate((w_low, jnp.float32(w_unit), w_high)):
            weight[plane, tile] = jnp.broadcast_to(w * factor, (ROWS, bx))
    total[...] = jnp.zeros(total.shape, jnp.float32)
    pairs[...] = jnp.zeros(pairs.shape, jnp.float32)

    for copy in owns + swaps:
        copy.wait()

    def z_copy(item, side):
        field, depth, k = item
        low_src, high_src = slice(S, S + depth), slice(S + bz - depth, S + bz)
        low_dst, high_dst = slice(S - depth, S), slice(S + bz, S + bz + depth)
        src, dst = ((low_src, high_dst), (high_src, low_dst))[side]
        return pltpu.make_async_remote_copy(
            src_ref=fields.at[field, src, :, mid_y, :], dst_ref=fields.at[field, dst, :, mid_y, :],
            send_sem=z_send.at[k, side], recv_sem=z_recv.at[k, 1 - side],
            device_id=z_dev[side], device_id_type=MESH)

    def y_copy(item, side, part):
        field, depth, k = item
        planes = (mid_z, slice(S - depth, S), slice(S + bz, S + bz + depth))[part]
        low_src, high_src = slice(first, first + depth), slice(first + hy - depth, first + hy)
        low_dst, high_dst = slice(first - depth, first), slice(first + hy, first + hy + depth)
        src, dst = ((low_src, high_dst), (high_src, low_dst))[side]
        return pltpu.make_async_remote_copy(
            src_ref=fields.at[field, planes, :, src, :], dst_ref=fields.at[field, planes, :, dst, :],
            send_sem=y_send.at[k, side, part], recv_sem=y_recv.at[k, 1 - side, part],
            device_id=y_dev[side], device_id_type=MESH)

    def exchange(shallow):
        items = ((1, S, 0), (shallow, S - 1, 1))
        for item in items:
            for side in range(2):
                @pl.when(has_z[side])
                def _():
                    z_copy(item, side).start()
        for item in items:
            for side in range(2):
                @pl.when(has_y[side])
                def _():
                    y_copy(item, side, 0).start()
        for item in items:
            for z_side in range(2):
                @pl.when(has_z[z_side])
                def _():
                    z_copy(item, 1 - z_side).wait_recv()
                    for side in range(2):
                        @pl.when(has_y[side])
                        def _():
                            y_copy(item, side, 1 + z_side).start()
        for item in items:
            for side in range(2):
                @pl.when(has_z[side])
                def _():
                    z_copy(item, side).wait_send()

                @pl.when(has_y[side])
                def _():
                    y_copy(item, side, 0).wait_send()
                    y_copy(item, 1 - side, 0).wait_recv()
                    for z_side in range(2):
                        @pl.when(has_z[z_side])
                        def _():
                            y_copy(item, side, 1 + z_side).wait_send()
                            y_copy(item, 1 - side, 1 + z_side).wait_recv()

    exchange(2)
    all_rows = slice(first - ROWS, first + hy + ROWS)

    def prepare(plane, c):
        fields[0, plane] = fields[1, plane]
        scale2[plane] = (fields[2, plane, :, all_rows, :] + (27.0 - SHIFT)) * (2.0 / HALF)
        return c
    lax.fori_loop(0, ze, prepare, 0)

    tiles = (hy + 2 * ROWS) // ROWS
    lane_id = lax.broadcasted_iota(jnp.int32, (ROWS, bx), 1)
    first_lane, last_lane = lane_id == 0, lane_id == bx - 1

    def row_sums(ref, z, tile):
        at = first - ROWS + tile * ROWS
        return [ref[z, h, at - 1:at - 1 + ROWS, :] + ref[z, h, at:at + ROWS, :] + ref[z, h, at + 1:at + 1 + ROWS, :]
                for h in range(halves)]

    def lane_sums(parts):
        left = [pltpu.roll(v, 1, 1) for v in parts]
        right = [pltpu.roll(v, bx - 1, 1) for v in parts]
        out = []
        for h in range(halves):
            before = left[h - 1] if h else 0.0
            after = right[h + 1] if h < halves - 1 else 0.0
            out.append(parts[h] + jnp.where(first_lane, before, left[h]) + jnp.where(last_lane, after, right[h]))
        return out

    p_at = [fields.at[1]] + [p_chain.at[k] for k in range(S)]
    r_at = [fields.at[0]] + [r_chain.at[k] for k in range(S - 1)]

    def degree_sweep(chains, degree, start, stop, chosen):
        jobs = [(chain, tile) for chain in chains for tile in chosen]

        def step(z, carry):
            out = []
            for (chain, tile), (before, here) in zip(jobs, carry):
                after = row_sums(chain[degree], z + 1, tile)
                box = lane_sums([a + b + c for a, b, c in zip(before, here, after)])
                at = first - ROWS + tile * ROWS
                for h in range(halves):
                    value = (scale2[z, h, tile * ROWS:(tile + 1) * ROWS, :] * chain[degree][z, h, at:at + ROWS, :]
                             - weight[z, tile] * box[h])
                    if degree == 0:
                        value = 0.5 * value
                    else:
                        value = value - chain[degree - 1][z, h, at:at + ROWS, :]
                    chain[degree + 1][z, h, at:at + ROWS, :] = value
                out.append((here, after))
            return tuple(out)
        init = tuple((row_sums(c[degree], start - 1, k), row_sums(c[degree], start, k)) for c, k in jobs)
        for z in range(start, stop):
            init = step(z, init)

    gl = lax.broadcasted_iota(jnp.int32, (2 * ROWS, LANES), 1)
    gr = lax.broadcasted_iota(jnp.int32, (2 * ROWS, LANES), 0)
    change = basis_change()
    diag_b = [change[i, i] for i in range(COLS)]
    low_b = [change[i, i - 1] if i else 0.0 for i in range(COLS)]
    up_b = [change[i, i + 1] if i < COLS - 1 else 0.0 for i in range(COLS)]
    b_row = [table(gl, v) for v in (diag_b, low_b, up_b)]
    b_col = [table(gr, v) for v in (diag_b, low_b, up_b)]

    b_down = [table(gl, v) for v in (
        diag_b, [change[j + 1, j] if j < COLS - 1 else 0.0 for j in range(COLS)],
        [change[j - 1, j] if j else 0.0 for j in range(COLS)])]

    def apply_b(col, row):
        q_row = b_row[0] * row + b_row[1] * pltpu.roll(row, 1, 1) + b_row[2] * pltpu.roll(row, LANES - 1, 1)
        q_col = b_col[0] * col + b_col[1] * pltpu.roll(col, 1, 0) + b_col[2] * pltpu.roll(col, 2 * ROWS - 1, 0)
        return q_col, q_row

    def outer(t, carry):
        for degree in range(S):
            if degree < S - 1:
                degree_sweep((p_at,), degree, degree + 1, ze - degree - 1, range(tiles))
                r_tiles = range(tiles) if degree < S - 2 else (1,)
                degree_sweep((r_at,), degree, degree + 2, ze - degree - 2, r_tiles)
            else:
                degree_sweep((p_at,), degree, degree + 1, ze - degree - 1, (1,))
        basis = p_at + r_at

        for lo_i, hi_i, lo_j in ((0, S + 1, 0), (0, S + 1, S + 1), (S + 1, COLS, S + 1)):
            hi_j = S + 1 if lo_j == 0 else COLS
            sums = {}
            for z in range(S, S + bz):
                for h in range(halves):
                    va = [basis[i][z, h, mid_y, :] for i in range(lo_i, hi_i)]
                    vb = va if lo_i == lo_j else [basis[j][z, h, mid_y, :] for j in range(lo_j, hi_j)]
                    for i in range(lo_i, hi_i):
                        for j in range(max(i, lo_j), hi_j):
                            term = va[i - lo_i] * vb[j - lo_j]
                            sums[i, j] = sums[i, j] + term if (i, j) in sums else term
            for (i, j), value in sums.items():
                line = jnp.sum(value, axis=0, keepdims=True)
                pairs[i * 16 + j:i * 16 + j + 1, :] = line
                if i != j:
                    pairs[j * 16 + i:j * 16 + i + 1, :] = line
        for half in range(2):
            turned = pairs[half * LANES:(half + 1) * LANES, :].T
            g_send[half:half + 1, :] = jnp.sum(turned, axis=0, keepdims=True)

        slot = t % 2
        turn = jnp.where(iz * 2 < nz, -1, 1)
        own = pltpu.make_async_copy(g_send, g_recv.at[slot, me], g_rsem.at[slot])
        own.start()

        def send(k, c):
            peer = (me + turn + turn * k + count) % count
            pltpu.make_async_remote_copy(
                src_ref=g_send, dst_ref=g_recv.at[slot, me],
                send_sem=g_ssem, recv_sem=g_rsem.at[slot],
                device_id=(peer // (ny * nx), (peer // nx) % ny, peer % nx), device_id_type=MESH).start()
            return c
        lax.fori_loop(0, count - 1, send, 0, unroll=4)
        everything = g_recv.at[slot]
        pltpu.make_async_copy(everything, everything, g_rsem.at[slot]).wait()
        most = g_recv.at[slot, 0:count - 1]
        pltpu.make_async_copy(most, most, g_ssem).wait()
        rows2 = jnp.sum(g_recv[slot], axis=0)
        gram = jnp.zeros((2 * ROWS, LANES), jnp.float32)
        for half in range(2):
            line = jnp.broadcast_to(rows2[half:half + 1, :], (2 * ROWS, LANES))
            for k in range(8):
                i = half * 8 + k
                if i < COLS:
                    moved = line if k == 0 else pltpu.roll(line, LANES - 16 * k, 1)
                    gram = jnp.where(gr == i, moved, gram)
        gram = jnp.where(gl < COLS, gram, 0.0)

        def quad(matrix, col, row):
            return jnp.sum(jnp.sum(matrix * col * row, axis=0, keepdims=True), axis=1, keepdims=True)

        moved_gram = (gram * b_down[0] + pltpu.roll(gram, LANES - 1, 1) * b_down[1] + pltpu.roll(gram, 1, 1) * b_down[2])

        p_row, p_col = (gl == 0).astype(jnp.float32), (gr == 0).astype(jnp.float32)
        r_row, r_col = (gl == S + 1).astype(jnp.float32), (gr == S + 1).astype(jnp.float32)
        x_col = jnp.zeros((2 * ROWS, LANES), jnp.float32)
        norm = quad(gram, r_col, r_row)
        for _ in range(S):
            q_col, q_row = apply_b(p_col, p_row)
            length = norm / quad(moved_gram, p_col, p_row)
            x_col = x_col + length * p_col
            r_col = r_col - length * q_col
            r_row = r_row - length * q_row
            fresh = quad(gram, r_col, r_row)
            ratio = fresh / norm
            p_col = r_col + ratio * p_col
            p_row = r_row + ratio * p_row
            norm = fresh

        def weights(col):
            return [jnp.broadcast_to(col[i:i + 1, :], (hy, LANES)) for i in range(COLS)]

        xw, rw, pw = weights(x_col), weights(r_col), weights(p_col)
        for z in range(bz):
            for h in range(halves):
                vs = [b[S + z, h, mid_y, :] for b in basis]

                def mix(w):
                    out = w[0] * vs[0]
                    for a, b in zip(w[1:], vs[1:]):
                        out = out + a * b
                    return out
                total[0, z, h] = total[0, z, h] + mix(xw)
                fields[0, S + z, h, mid_y, :] = mix(rw)
                fields[1, S + z, h, mid_y, :] = mix(pw)

        @pl.when(t < OUTER - 1)
        def _():
            exchange(0)
        return carry

    lax.fori_loop(0, OUTER, outer, 0)

    total[1] = fields[0, mid_z, :, mid_y, :]
    back = pltpu.make_async_remote_copy(
        src_ref=total.at[:, :, other], dst_ref=final,
        send_sem=swap_send.at[0], recv_sem=swap_recv.at[0],
        device_id=(iz, iy, other), device_id_type=MESH)
    back.start()
    for k, out in enumerate((sol_out, res_out)):
        out[:, row_tile(ix), :] = total[k, :, ix]
    back.wait()
    for k, out in enumerate((sol_out, res_out)):
        out[:, row_tile(other), :] = final[k]


def solution(mesh):
    nz, ny, nx = mesh.shape["gz"], mesh.shape["gy"], mesh.shape["gx"]
    count = nz * ny * nx

    def body(right_side, diagonal):
        bz, by, bx = right_side.shape
        hy = by // 2
        assert nx == 2 and bz >= S and hy == ROWS and bx == LANES
        ze, ye = bz + 2 * S, hy + 4 * ROWS
        f32, dma = jnp.float32, pltpu.SemaphoreType.DMA
        return pl.pallas_call(
            lambda *refs: kernel(nz, ny, nx, *refs),
            out_shape=(jax.ShapeDtypeStruct(right_side.shape, f32),) * 2,
            in_specs=[pl.BlockSpec(memory_space=pltpu.VMEM)] * 2,
            out_specs=(pl.BlockSpec(memory_space=pltpu.VMEM),) * 2,
            scratch_shapes=[
                pltpu.VMEM((3, ze, nx, ye, bx), f32),
                pltpu.VMEM((S, ze, nx, ye, bx), f32),
                pltpu.VMEM((S - 1, ze, nx, ye, bx), f32),
                pltpu.VMEM((ze, nx, hy + 2 * ROWS, bx), f32),
                pltpu.VMEM((ze, 3, ROWS, bx), f32),
                pltpu.VMEM((2, bz, nx, hy, bx), f32),
                pltpu.VMEM((2 * LANES, LANES), f32),
                pltpu.VMEM((2, LANES), f32),
                pltpu.VMEM((2, count, 2, LANES), f32),
                pltpu.VMEM((2, bz, hy, bx), f32),
                dma((2, 2)), dma((2, 2)), dma((2, 2, 3)), dma((2, 2, 3)),
                dma, dma((2,)), dma((2,)), dma((2,)), dma((2,)),
            ],
            compiler_params=pltpu.CompilerParams(has_side_effects=True),
        )(right_side, diagonal)

    spec = P("gz", "gy", "gx")
    return jax.shard_map(body, mesh=mesh, in_specs=(spec, spec), out_specs=(spec, spec), check_vma=False)
```

```python
import jax
import jax.numpy as jnp
import numpy as np
from jax import lax
from jax.experimental import pallas as pl
from jax.experimental.pallas import tpu as pltpu
from jax.sharding import PartitionSpec as P

S = 6
OUTER = 5
COLS = 2 * S + 1
SHIFT = 19.0
HALF = 19.0
LANES = 128
ROWS = 8
MESH = pl.DeviceIdType.MESH


def basis_change():
    matrix = np.zeros((COLS, COLS), np.float32)
    for offset, length in ((0, S), (S + 1, S - 1)):
        for degree in range(length):
            matrix[offset + degree, offset + degree] = SHIFT
            if degree == 0:
                matrix[offset + 1, offset] = HALF
            else:
                matrix[offset + degree + 1, offset + degree] = 0.5 * HALF
                matrix[offset + degree - 1, offset + degree] = 0.5 * HALF
    return matrix


def table(index, values):
    out = jnp.zeros(index.shape, jnp.float32)
    for position, value in enumerate(values):
        if value:
            out = jnp.where(index == position, jnp.float32(value), out)
    return out


def kernel(nz, ny, nx, rhs_ref, diag_ref, sol_out, res_out,
           fields, p_chain, r_chain, scale2, weight, total, pairs, g_send, g_recv, final, kept,
           z_send, z_recv, y_send, y_recv, g_ssem, g_rsem, swap_send, swap_recv, own_sem):
    bz, by, bx = rhs_ref.shape
    hy = by // 2
    ze, halves, ya = fields.shape[1:4]
    first = (ya - hy) // 2
    low_rows, high_rows = slice(first - ROWS, first), slice(first + hy, first + hy + ROWS)
    iz, iy, ix = lax.axis_index("gz"), lax.axis_index("gy"), lax.axis_index("gx")
    other = 1 - ix
    yy = iy * 2 + ix
    count = nz * ny * nx
    me = (iz * ny + iy) * nx + ix
    has_z = (iz > 0, iz < nz - 1)
    has_y = (yy > 0, yy < 2 * ny - 1)
    z_dev = tuple((iz + s, iy, ix) for s in (-1, 1))
    y_dev = tuple((iz, (yy + s) // 2, other) for s in (-1, 1))
    mid_z, mid_y = slice(S, S + bz), slice(first, first + hy)

    def row_tile(index):
        return pl.ds(pl.multiple_of(index * hy, hy), hy)

    swaps, owns = [], []
    for k, ref in enumerate((rhs_ref, diag_ref)):
        spot = fields.at[1 + k, mid_z, ix, mid_y, :]
        swap = pltpu.make_async_remote_copy(
            src_ref=ref.at[:, row_tile(other), :], dst_ref=spot,
            send_sem=swap_send.at[k], recv_sem=swap_recv.at[k],
            device_id=(iz, iy, other), device_id_type=MESH)
        swap.start()
        own = pltpu.make_async_copy(ref.at[:, row_tile(ix), :], spot, own_sem.at[k])
        own.start()
        swaps.append(swap)
        owns.append(own)

    for side in range(2):
        planes = slice(0, S) if side == 0 else slice(S + bz, ze)
        rows = (low_rows, high_rows)[side]

        @pl.when(jnp.logical_not(has_z[side]))
        def _():
            for k in (0, 1, 2):
                fields[k, planes] = jnp.zeros((S, halves, ya, bx), jnp.float32)

        @pl.when(jnp.logical_not(has_y[side]))
        def _():
            for k in (0, 1, 2):
                fields[k, :, :, rows, :] = jnp.zeros((ze, halves, ROWS, bx), jnp.float32)

    w_unit = 2.0 / HALF
    w_low = jnp.where(has_y[0], jnp.float32(w_unit), 0.0)
    w_high = jnp.where(has_y[1], jnp.float32(w_unit), 0.0)
    z_low = jnp.where(has_z[0], jnp.float32(1.0), 0.0)
    z_high = jnp.where(has_z[1], jnp.float32(1.0), 0.0)
    for plane in range(ze):
        factor = z_low if plane < S else (z_high if plane >= S + bz else jnp.float32(1.0))
        for tile, w in enumerate((w_low, jnp.float32(w_unit), w_high)):
            weight[plane, tile] = jnp.broadcast_to(w * factor, (ROWS, bx))
    total[...] = jnp.zeros(total.shape, jnp.float32)
    pairs[...] = jnp.zeros(pairs.shape, jnp.float32)

    for copy in owns + swaps:
        copy.wait()

    def z_copy(item, side):
        field, depth, k = item
        low_src, high_src = slice(S, S + depth), slice(S + bz - depth, S + bz)
        low_dst, high_dst = slice(S - depth, S), slice(S + bz, S + bz + depth)
        src, dst = ((low_src, high_dst), (high_src, low_dst))[side]
        return pltpu.make_async_remote_copy(
            src_ref=fields.at[field, src, :, mid_y, :], dst_ref=fields.at[field, dst, :, mid_y, :],
            send_sem=z_send.at[k, side], recv_sem=z_recv.at[k, 1 - side],
            device_id=z_dev[side], device_id_type=MESH)

    def y_copy(item, side, part):
        field, depth, k = item
        planes = (mid_z, slice(S - depth, S), slice(S + bz, S + bz + depth))[part]
        low_src, high_src = slice(first, first + depth), slice(first + hy - depth, first + hy)
        low_dst, high_dst = slice(first - depth, first), slice(first + hy, first + hy + depth)
        src, dst = ((low_src, high_dst), (high_src, low_dst))[side]
        return pltpu.make_async_remote_copy(
            src_ref=fields.at[field, planes, :, src, :], dst_ref=fields.at[field, planes, :, dst, :],
            send_sem=y_send.at[k, side, part], recv_sem=y_recv.at[k, 1 - side, part],
            device_id=y_dev[side], device_id_type=MESH)

    def start(item):
        for side in range(2):
            @pl.when(has_z[side])
            def _():
                z_copy(item, side).start()
        for side in range(2):
            @pl.when(has_y[side])
            def _():
                y_copy(item, side, 0).start()

    def finish(items):
        for item in items:
            for z_side in range(2):
                @pl.when(has_z[z_side])
                def _():
                    z_copy(item, 1 - z_side).wait_recv()
                    for side in range(2):
                        @pl.when(has_y[side])
                        def _():
                            y_copy(item, side, 1 + z_side).start()
        for item in items:
            for side in range(2):
                @pl.when(has_z[side])
                def _():
                    z_copy(item, side).wait_send()

                @pl.when(has_y[side])
                def _():
                    y_copy(item, side, 0).wait_send()
                    y_copy(item, 1 - side, 0).wait_recv()
                    for z_side in range(2):
                        @pl.when(has_z[z_side])
                        def _():
                            y_copy(item, side, 1 + z_side).wait_send()
                            y_copy(item, 1 - side, 1 + z_side).wait_recv()

    start((1, S, 0))
    start((2, S - 1, 1))
    finish(((1, S, 0), (2, S - 1, 1)))
    all_rows = slice(first - ROWS, first + hy + ROWS)

    def prepare(plane, c):
        fields[0, plane] = fields[1, plane]
        scale2[plane] = (fields[2, plane, :, all_rows, :] + (27.0 - SHIFT)) * (2.0 / HALF)
        return c
    lax.fori_loop(0, ze, prepare, 0)

    tiles = (hy + 2 * ROWS) // ROWS
    lane_id = lax.broadcasted_iota(jnp.int32, (ROWS, bx), 1)
    first_lane, last_lane = lane_id == 0, lane_id == bx - 1

    def row_sums(ref, z, tile):
        at = first - ROWS + tile * ROWS
        return [ref[z, h, at - 1:at - 1 + ROWS, :] + ref[z, h, at:at + ROWS, :] + ref[z, h, at + 1:at + 1 + ROWS, :]
                for h in range(halves)]

    def lane_sums(parts):
        left = [pltpu.roll(v, 1, 1) for v in parts]
        right = [pltpu.roll(v, bx - 1, 1) for v in parts]
        out = []
        for h in range(halves):
            before = left[h - 1] if h else 0.0
            after = right[h + 1] if h < halves - 1 else 0.0
            out.append(parts[h] + jnp.where(first_lane, before, left[h]) + jnp.where(last_lane, after, right[h]))
        return out

    p_at = [fields.at[1]] + [p_chain.at[k] for k in range(S)]
    r_at = [fields.at[0]] + [r_chain.at[k] for k in range(S - 1)]

    def degree_sweep(chains, degree, start, stop, chosen):
        jobs = [(chain, tile) for chain in chains for tile in chosen]

        def step(z, carry):
            out = []
            for (chain, tile), (before, here) in zip(jobs, carry):
                after = row_sums(chain[degree], z + 1, tile)
                box = lane_sums([a + b + c for a, b, c in zip(before, here, after)])
                at = first - ROWS + tile * ROWS
                for h in range(halves):
                    value = (scale2[z, h, tile * ROWS:(tile + 1) * ROWS, :] * chain[degree][z, h, at:at + ROWS, :]
                             - weight[z, tile] * box[h])
                    if degree == 0:
                        value = 0.5 * value
                    else:
                        value = value - chain[degree - 1][z, h, at:at + ROWS, :]
                    chain[degree + 1][z, h, at:at + ROWS, :] = value
                out.append((here, after))
            return tuple(out)
        init = tuple((row_sums(c[degree], start - 1, k), row_sums(c[degree], start, k)) for c, k in jobs)
        for z in range(start, stop):
            init = step(z, init)

    gl = lax.broadcasted_iota(jnp.int32, (2 * ROWS, LANES), 1)
    gr = lax.broadcasted_iota(jnp.int32, (2 * ROWS, LANES), 0)
    change = basis_change()
    diag_b = [change[i, i] for i in range(COLS)]
    low_b = [change[i, i - 1] if i else 0.0 for i in range(COLS)]
    up_b = [change[i, i + 1] if i < COLS - 1 else 0.0 for i in range(COLS)]
    b_row = [table(gl, v) for v in (diag_b, low_b, up_b)]
    b_col = [table(gr, v) for v in (diag_b, low_b, up_b)]

    b_down = [table(gl, v) for v in (
        diag_b, [change[j + 1, j] if j < COLS - 1 else 0.0 for j in range(COLS)],
        [change[j - 1, j] if j else 0.0 for j in range(COLS)])]

    def apply_b(col, row):
        q_row = b_row[0] * row + b_row[1] * pltpu.roll(row, 1, 1) + b_row[2] * pltpu.roll(row, LANES - 1, 1)
        q_col = b_col[0] * col + b_col[1] * pltpu.roll(col, 1, 0) + b_col[2] * pltpu.roll(col, 2 * ROWS - 1, 0)
        return q_col, q_row

    def outer(t, carry):
        for degree in range(S):
            if degree < S - 1:
                degree_sweep((p_at,), degree, degree + 1, ze - degree - 1, range(tiles))
                r_tiles = range(tiles) if degree < S - 2 else (1,)
                degree_sweep((r_at,), degree, degree + 2, ze - degree - 2, r_tiles)
            else:
                degree_sweep((p_at,), degree, degree + 1, ze - degree - 1, (1,))
        basis = p_at + r_at

        for lo_i, hi_i, lo_j in ((0, S + 1, 0), (0, S + 1, S + 1), (S + 1, COLS, S + 1)):
            hi_j = S + 1 if lo_j == 0 else COLS
            sums = {}
            for z in range(S, S + bz):
                for h in range(halves):
                    va = [basis[i][z, h, mid_y, :] for i in range(lo_i, hi_i)]
                    vb = va if lo_i == lo_j else [basis[j][z, h, mid_y, :] for j in range(lo_j, hi_j)]
                    for i in range(lo_i, hi_i):
                        for j in range(max(i, lo_j), hi_j):
                            term = va[i - lo_i] * vb[j - lo_j]
                            sums[i, j] = sums[i, j] + term if (i, j) in sums else term
            for (i, j), value in sums.items():
                line = jnp.sum(value, axis=0, keepdims=True)
                pairs[i * 16 + j:i * 16 + j + 1, :] = line
                if i != j:
                    pairs[j * 16 + i:j * 16 + i + 1, :] = line
        for half in range(2):
            turned = pairs[half * LANES:(half + 1) * LANES, :].T
            g_send[half:half + 1, :] = jnp.sum(turned, axis=0, keepdims=True)

        slot = t % 2
        turn = jnp.where(iz * 2 < nz, -1, 1)
        own = pltpu.make_async_copy(g_send, g_recv.at[slot, me], g_rsem.at[slot])
        own.start()

        def send(k, c):
            peer = (me + turn + turn * k + count) % count
            pltpu.make_async_remote_copy(
                src_ref=g_send, dst_ref=g_recv.at[slot, me],
                send_sem=g_ssem, recv_sem=g_rsem.at[slot],
                device_id=(peer // (ny * nx), (peer // nx) % ny, peer % nx), device_id_type=MESH).start()
            return c
        lax.fori_loop(0, count - 1, send, 0, unroll=4)
        for k in range(2):
            kept[k] = fields[1 - k, mid_z, :, mid_y, :]
        everything = g_recv.at[slot]
        pltpu.make_async_copy(everything, everything, g_rsem.at[slot]).wait()
        most = g_recv.at[slot, 0:count - 1]
        pltpu.make_async_copy(most, most, g_ssem).wait()
        rows2 = jnp.sum(g_recv[slot], axis=0)
        gram = jnp.zeros((2 * ROWS, LANES), jnp.float32)
        for half in range(2):
            line = jnp.broadcast_to(rows2[half:half + 1, :], (2 * ROWS, LANES))
            for k in range(8):
                i = half * 8 + k
                if i < COLS:
                    moved = line if k == 0 else pltpu.roll(line, LANES - 16 * k, 1)
                    gram = jnp.where(gr == i, moved, gram)
        gram = jnp.where(gl < COLS, gram, 0.0)

        def quad(matrix, col, row):
            return jnp.sum(jnp.sum(matrix * col * row, axis=0, keepdims=True), axis=1, keepdims=True)

        moved_gram = (gram * b_down[0] + pltpu.roll(gram, LANES - 1, 1) * b_down[1] + pltpu.roll(gram, 1, 1) * b_down[2])

        p_row, p_col = (gl == 0).astype(jnp.float32), (gr == 0).astype(jnp.float32)
        r_row, r_col = (gl == S + 1).astype(jnp.float32), (gr == S + 1).astype(jnp.float32)
        x_col = jnp.zeros((2 * ROWS, LANES), jnp.float32)
        norm = quad(gram, r_col, r_row)
        for _ in range(S):
            q_col, q_row = apply_b(p_col, p_row)
            length = norm / quad(moved_gram, p_col, p_row)
            x_col = x_col + length * p_col
            r_col = r_col - length * q_col
            r_row = r_row - length * q_row
            fresh = quad(gram, r_col, r_row)
            ratio = fresh / norm
            p_col = r_col + ratio * p_col
            p_row = r_row + ratio * p_row
            norm = fresh

        def weights(col):
            return [jnp.broadcast_to(col[i:i + 1, :], (hy, LANES)) for i in range(COLS)]

        xw, rw, pw = weights(x_col), weights(r_col), weights(p_col)
        cells = [(z, h) for z in range(bz) for h in range(halves)]

        def mix(w, z, h):
            vs = [kept[0, z, h]] + [b[S + z, h, mid_y, :] for b in p_at[1:]]
            vs += [kept[1, z, h]] + [b[S + z, h, mid_y, :] for b in r_at[1:]]
            out = w[0] * vs[0]
            for a, b in zip(w[1:], vs[1:]):
                out = out + a * b
            return out

        items = ((1, S, 0), (0, S - 1, 1))
        for item, w in zip(items, (pw, rw)):
            for z, h in cells:
                fields[item[0], S + z, h, mid_y, :] = mix(w, z, h)

            @pl.when(t < OUTER - 1)
            def _():
                start(item)
        for z, h in cells:
            total[0, z, h] = total[0, z, h] + mix(xw, z, h)

        @pl.when(t < OUTER - 1)
        def _():
            finish(items)
        return carry

    lax.fori_loop(0, OUTER, outer, 0)

    total[1] = fields[0, mid_z, :, mid_y, :]
    back = pltpu.make_async_remote_copy(
        src_ref=total.at[:, :, other], dst_ref=final,
        send_sem=swap_send.at[0], recv_sem=swap_recv.at[0],
        device_id=(iz, iy, other), device_id_type=MESH)
    back.start()
    for k, out in enumerate((sol_out, res_out)):
        out[:, row_tile(ix), :] = total[k, :, ix]
    back.wait()
    for k, out in enumerate((sol_out, res_out)):
        out[:, row_tile(other), :] = final[k]


def solution(mesh):
    nz, ny, nx = mesh.shape["gz"], mesh.shape["gy"], mesh.shape["gx"]
    count = nz * ny * nx

    def body(right_side, diagonal):
        bz, by, bx = right_side.shape
        hy = by // 2
        assert nx == 2 and bz >= S and hy == ROWS and bx == LANES
        ze, ye = bz + 2 * S, hy + 4 * ROWS
        f32, dma = jnp.float32, pltpu.SemaphoreType.DMA
        return pl.pallas_call(
            lambda *refs: kernel(nz, ny, nx, *refs),
            out_shape=(jax.ShapeDtypeStruct(right_side.shape, f32),) * 2,
            in_specs=[pl.BlockSpec(memory_space=pltpu.VMEM)] * 2,
            out_specs=(pl.BlockSpec(memory_space=pltpu.VMEM),) * 2,
            scratch_shapes=[
                pltpu.VMEM((3, ze, nx, ye, bx), f32),
                pltpu.VMEM((S, ze, nx, ye, bx), f32),
                pltpu.VMEM((S - 1, ze, nx, ye, bx), f32),
                pltpu.VMEM((ze, nx, hy + 2 * ROWS, bx), f32),
                pltpu.VMEM((ze, 3, ROWS, bx), f32),
                pltpu.VMEM((2, bz, nx, hy, bx), f32),
                pltpu.VMEM((2 * LANES, LANES), f32),
                pltpu.VMEM((2, LANES), f32),
                pltpu.VMEM((2, count, 2, LANES), f32),
                pltpu.VMEM((2, bz, hy, bx), f32),
                pltpu.VMEM((2, bz, nx, hy, bx), f32),
                dma((2, 2)), dma((2, 2)), dma((2, 2, 3)), dma((2, 2, 3)),
                dma, dma((2,)), dma((2,)), dma((2,)), dma((2,)),
            ],
            compiler_params=pltpu.CompilerParams(has_side_effects=True),
        )(right_side, diagonal)

    spec = P("gz", "gy", "gx")
    return jax.shard_map(body, mesh=mesh, in_specs=(spec, spec), out_specs=(spec, spec), check_vma=False)
```
